512 devices in a mesh: task: 4 (over z_hi, core), seq: 16 (over x, y), dp: 8 (over z_lo).
Axes of the slice: x: 4, y: 4, z: 16 (z_hi: 2, z_lo: 8; z = z_hi * 8 + z_lo), core: 2. Of those that a mesh axis runs over, the one named last changes fastest.
Arguments:
- enc_grads: bfloat16 [4, 8, 2048, 4096], P('task', 'dp', 'seq'), may hold values from -12 to 12
- hidden: bfloat16 [8, 2048, 4096], P('dp', 'seq', 'task'), may hold values from -900 to 900
- final_gain: float32 [4096], replicated, may hold values from 0.1 to 1.9
- attn_out: bfloat16 [8, 2048, 4096], P('dp', 'seq', 'task'), may hold values from -6 to 6
- qkv: bfloat16 [8, 2048, 64, 192], P('dp', None, ('task', 'seq')), may hold values from -48 to 48
- out_weight: bfloat16 [4096, 4096], P('task', ('seq', 'dp')), may hold values from -0.09375 to 0.09375
- doc_lengths: int32 [8], P('dp'), may hold values from 512 to 2048
Outputs:
- resid_grad: bfloat16 [8, 2048, 4096], P('dp', 'seq', 'task')
- qkv_grad: bfloat16 [8, 2048, 64, 192], P('dp', None, ('task', 'seq'))
- weight_grad: float32 [4096, 4096], P('task', ('seq', 'dp'))
The draws below stay inside these ranges and needn't reach their ends.
Inputs may be any that keep to these rules, and one draw needn't show every extreme that they name: `doc_lengths`: positions at or after a document's length are padding and are never attended to as keys.
All inputs are finite; a program needn't handle non-finite values.
Results may differ from the reference program's by a relative error of at most 0.02.
Values may be sent and summed in bfloat16 or wider, within the bound.
No kernel may reach another device: no remote copies, remote signals or barrier semaphores. Data moves between devices by JAX's collectives and lax.ppermute only.
A program may use at most 64 MiB of HBM per device.

```python
import math
import jax
import jax.numpy as jnp
from jax import lax

D = 4096
HEADS = 64
DH = 64
LEN = 2048
DOCS = 8
HD = 4096
N_TASK = 4


def draw_hidden(key, part):
    first, second, third = jax.random.split(jax.random.fold_in(key, 11), 3)
    row_scale = jnp.exp(jax.random.uniform(first, (DOCS, LEN, 1), minval=0.0, maxval=math.log(10.0)))
    ramp = jnp.arange(D, dtype=jnp.float32) / D
    col_scale = jnp.exp(math.log(10.0) * ramp + jax.random.uniform(second, (D,), minval=-0.35, maxval=0.35))
    base = jnp.clip(jax.random.normal(third, (DOCS, LEN, D)), -6.0, 6.0)
    return (base * row_scale * col_scale).astype(jnp.bfloat16)


def draw_qkv(key, part):
    keys_all = jax.random.split(jax.random.fold_in(key, 23), 1)
    spread = DH ** (-0.25)
    base = spread * jnp.clip(jax.random.normal(keys_all[0], (DOCS, LEN, HEADS, 3 * DH)), -6.0, 6.0)
    return base.astype(jnp.bfloat16)


def with_ends(drawn, own_key, smallest, high):
    place = [jax.random.randint(jax.random.fold_in(own_key, axis), (), 0, length) for axis, length in enumerate(drawn.shape)]
    longest = drawn.shape.index(max(drawn.shape))
    next_to = place[:longest] + [(place[longest] + 1) % drawn.shape[longest]] + place[longest + 1:]
    return drawn.at[tuple(place)].set(smallest).at[tuple(next_to)].set(high)


def block_scale(key, extent, cuts, least, largest):
    def one(axis_at, shards_of):
        draws = jax.random.uniform(jax.random.fold_in(jax.random.fold_in(key, 6), axis_at), (shards_of,), jnp.float32, least / len(cuts), largest / len(cuts))
        return jnp.repeat(jnp.exp(draws), extent[axis_at] // shards_of).reshape((-1,) + (1,) * (len(extent) - axis_at - 1))

    gain = one(*cuts[0])
    for cut in cuts[1:]:
        gain = gain * one(*cut)
    return gain


def gaussian(key, dims, scale, reach, shards=(), held_as=jnp.bfloat16):
    values = scale * jax.random.normal(key, dims, jnp.float32)
    if shards:
        values = values * block_scale(key, dims, shards, -0.22, 0.18)
    return jnp.clip(values, -reach, reach).astype(held_as)


def setup_inputs(seed: int = 0) -> dict:
    seeds = jax.random.split(jax.random.key(seed), 8)
    return {
        "enc_grads": gaussian(seeds[0], (N_TASK, DOCS, LEN, D), 2.0, 12.0, ((0, 4), (1, 8), (2, 16))),
        "hidden": draw_hidden(jax.random.fold_in(seeds[7], 71), 0),
        "final_gain": jnp.clip(1.0 + 0.18 * jax.random.normal(seeds[2], (D,), jnp.float32), 0.1, 1.9),
        "attn_out": gaussian(seeds[3], (DOCS, LEN, HD), 1.0, 6.0, ((0, 8), (1, 16), (2, 4))),
        "qkv": draw_qkv(jax.random.fold_in(seeds[7], 71), 0),
        "out_weight": gaussian(seeds[5], (HD, D), D ** -0.5, 0.09375, ((0, 4), (1, 128))),
        "doc_lengths": with_ends(jax.random.randint(seeds[6], (DOCS,), LEN // 4, LEN + 1), jax.random.fold_in(seeds[6], 1), LEN // 4, LEN).astype(jnp.int32),
    }


eps_norm = 1e-06

def attend(query, key_rows, value_rows, upstream, delta_rows, doc_length):
    key_valid = jnp.arange(query.shape[0], dtype=jnp.int32) < doc_length.astype(jnp.int32)
    scores = lax.dot_general(query, key_rows, (((1,), (1,)), ((), ())), preferred_element_type=jnp.float32)
    scores = jnp.where(key_valid[None, :], scores, -1e+30)
    row_max = lax.optimization_barrier(jnp.max(scores, axis=-1, keepdims=True))
    expo_terms = jnp.exp(scores - row_max)
    prob_rows = expo_terms / lax.optimization_barrier(jnp.sum(expo_terms, axis=-1, keepdims=True))
    prob_bf16 = prob_rows.astype(jnp.bfloat16)
    dvalue = lax.dot_general(prob_bf16, upstream, (((0,), (0,)), ((), ())), preferred_element_type=jnp.float32)
    dprob_rows = lax.dot_general(upstream, value_rows, (((1,), (1,)), ((), ())), preferred_element_type=jnp.float32)
    dscore_rows = (prob_rows * (dprob_rows - delta_rows[:, None])).astype(jnp.bfloat16)
    dquery = jnp.dot(dscore_rows, key_rows, preferred_element_type=jnp.float32)
    dkey = lax.dot_general(dscore_rows, query, (((0,), (0,)), ((), ())), preferred_element_type=jnp.float32)
    return jnp.concatenate([dquery.astype(jnp.bfloat16), dkey.astype(jnp.bfloat16), dvalue.astype(jnp.bfloat16)], axis=-1)

def reference(enc_grads, hidden, final_gain, attn_out, qkv, out_weight, doc_lengths):
    gsum = lax.optimization_barrier(jnp.sum(enc_grads.astype(jnp.float32), axis=0))
    stream = hidden.astype(jnp.float32)
    rstd = lax.rsqrt(lax.optimization_barrier(jnp.mean(stream * stream, axis=-1, keepdims=True)) + eps_norm)
    normed = stream * rstd
    cross_mean = lax.optimization_barrier(jnp.mean(final_gain * gsum * normed, axis=-1, keepdims=True))
    resid_grad = (rstd * (final_gain * gsum - normed * cross_mean)).astype(jnp.bfloat16)
    head_grad = jnp.einsum('ntd,ad->nta', resid_grad.astype(jnp.float32), out_weight.astype(jnp.float32)).astype(jnp.bfloat16)
    grad_view = head_grad.reshape(DOCS, LEN, HEADS, DH)
    saved_view = attn_out.reshape(DOCS, LEN, HEADS, DH)
    delta = lax.optimization_barrier(jnp.sum(grad_view.astype(jnp.float32) * saved_view.astype(jnp.float32), axis=-1))
    packed = jnp.transpose(qkv, (0, 2, 1, 3)).reshape(DOCS * HEADS, LEN, 3 * DH)
    upstream_all = jnp.transpose(grad_view, (0, 2, 1, 3)).reshape(DOCS * HEADS, LEN, DH)
    delta_all = jnp.transpose(delta, (0, 2, 1)).reshape(DOCS * HEADS, LEN)
    length_all = jnp.repeat(doc_lengths.astype(jnp.int32), HEADS)

    def one_head(items):
        packed_head, upstream, delta_rows, doc_length = items
        return attend(packed_head[:, :DH], packed_head[:, DH:2 * DH], packed_head[:, 2 * DH:], upstream, delta_rows, doc_length)
    results = lax.map(one_head, (packed, upstream_all, delta_all, length_all))
    qkv_grad = jnp.transpose(results.reshape(DOCS, HEADS, LEN, 3 * DH), (0, 2, 1, 3))
    weight_grad = jnp.einsum('nta,ntb->ab', attn_out.astype(jnp.float32), resid_grad.astype(jnp.float32))
    return (resid_grad, qkv_grad, weight_grad)
```

```python
import jax
import jax.numpy as jnp
from jax import lax
from jax.experimental import pallas as pl
from jax.experimental.pallas import tpu as pltpu
from jax.sharding import PartitionSpec as P


eps_norm = 1e-06
core_swap = [(0, 1), (1, 0), (2, 3), (3, 2)]
far_swap = [(0, 2), (2, 0), (1, 3), (3, 1)]
corner_swap = [(0, 3), (3, 0), (1, 2), (2, 1)]
NT = (((1,), (1,)), ((), ()))
NN = (((1,), (0,)), ((), ()))
tile = 256


def probs_kernel(length_ref, q_ref, k_ref, out_ref, held):
    keys = k_ref.shape[0]
    q = q_ref[...]
    length = length_ref[0]
    top = None
    for start in range(0, keys, tile):
        rows = pl.ds(start, tile)
        s = lax.dot_general(k_ref[rows, :], q, NT, preferred_element_type=jnp.float32)
        place = lax.broadcasted_iota(jnp.int32, s.shape, 0) + start
        s = jnp.where(place < length, s, -1e30)
        held[rows, :] = s
        peak = jnp.max(s, axis=0, keepdims=True)
        top = peak if top is None else jnp.maximum(top, peak)
    total = jnp.zeros_like(top)
    for start in range(0, keys, tile):
        rows = pl.ds(start, tile)
        e = jnp.exp(held[rows, :] - top)
        held[rows, :] = e
        total = total + jnp.sum(e, axis=0, keepdims=True)
    share = 1.0 / total
    for start in range(0, keys, tile):
        rows = pl.ds(start, tile)
        out_ref[rows, :] = (held[rows, :] * share).astype(out_ref.dtype)


def probs_of(length, query, key_rows):
    n, size = query.shape
    return pl.pallas_call(
        probs_kernel,
        grid=(n // tile,),
        in_specs=[
            pl.BlockSpec(memory_space=pltpu.SMEM),
            pl.BlockSpec((tile, size), lambda i: (i, 0)),
            pl.BlockSpec((n, size), lambda i: (0, 0)),
        ],
        out_specs=pl.BlockSpec((n, tile), lambda i: (0, i)),
        out_shape=jax.ShapeDtypeStruct((n, n), jnp.bfloat16),
        scratch_shapes=[pltpu.VMEM((n, tile), jnp.float32)],
        cost_estimate=pl.CostEstimate(
            flops=8 * n * n * size, bytes_accessed=2 * n * n, transcendentals=n * n
        ),
        name="probs",
    )(length, query, key_rows)


def grads_kernel(p_ref, q_ref, g_ref, o_ref, k_ref, v_ref, kt_ref, out_ref, dk_acc, dv_acc):
    i = pl.program_id(0)
    keys, size = k_ref.shape
    q = q_ref[...]
    g = g_ref[...]
    prod = g.astype(jnp.float32) * o_ref[...].astype(jnp.float32)
    delta = lax.dot_general(
        jnp.ones((8, size), jnp.float32),
        prod,
        NT,
        precision=lax.Precision.HIGHEST,
        preferred_element_type=jnp.float32,
    )[0:1, :]

    @pl.when(i == 0)
    def _():
        dk_acc[...] = jnp.zeros_like(dk_acc)
        dv_acc[...] = jnp.zeros_like(dv_acc)

    dqt = jnp.zeros((size, tile), jnp.float32)
    for start in range(0, keys, tile):
        rows = pl.ds(start, tile)
        p = p_ref[rows, :]
        dp = lax.dot_general(v_ref[rows, :], g, NT, preferred_element_type=jnp.float32)
        ds = (p.astype(jnp.float32) * (dp - delta)).astype(jnp.bfloat16)
        dv_acc[rows, :] += lax.dot_general(p, g, NN, preferred_element_type=jnp.float32)
        dk_acc[rows, :] += lax.dot_general(ds, q, NN, preferred_element_type=jnp.float32)
        dqt = dqt + lax.dot_general(kt_ref[:, rows], ds, NN, preferred_element_type=jnp.float32)
    out_ref[pl.ds(pl.multiple_of(i * tile, tile), tile), 0:size] = dqt.T.astype(out_ref.dtype)

    @pl.when(i == pl.num_programs(0) - 1)
    def _():
        out_ref[:, size : 2 * size] = dk_acc[...].astype(out_ref.dtype)
        out_ref[:, 2 * size :] = dv_acc[...].astype(out_ref.dtype)


def grads_of(probs, query, upstream, saved, key_rows, value_rows, key_cols):
    n, size = query.shape
    part = pl.BlockSpec((tile, size), lambda i: (i, 0))
    whole = pl.BlockSpec((n, size), lambda i: (0, 0))
    return pl.pallas_call(
        grads_kernel,
        grid=(n // tile,),
        in_specs=[
            pl.BlockSpec((n, tile), lambda i: (0, i)),
            part,
            part,
            part,
            whole,
            whole,
            pl.BlockSpec((size, n), lambda i: (0, 0)),
        ],
        out_specs=pl.BlockSpec((n, 3 * size), lambda i: (0, 0)),
        out_shape=jax.ShapeDtypeStruct((n, 3 * size), jnp.bfloat16),
        scratch_shapes=[pltpu.VMEM((n, size), jnp.float32), pltpu.VMEM((n, size), jnp.float32)],
        cost_estimate=pl.CostEstimate(
            flops=8 * n * n * size, bytes_accessed=2 * n * n, transcendentals=0
        ),
        name="grads",
    )(probs, query, upstream, saved, key_rows, value_rows, key_cols)


def copy_for_each(shard, axis):
    copies = jnp.broadcast_to(shard, (lax.axis_size(axis), *shard.shape))
    return lax.all_to_all(copies, axis, split_axis=0, concat_axis=0, tiled=True)


def pick(stack, index):
    return lax.dynamic_index_in_dim(stack, index, 0, keepdims=False)


def compute(enc_grads, hidden, final_gain, attn_out, qkv, out_weight, doc_lengths):
    rows, feature_cols = enc_grads.shape[2:]
    tasks = lax.axis_size("task")
    task_pos = lax.axis_index("task")
    far, core = task_pos // 2, task_pos % 2
    share_cols = feature_cols // tasks
    dp_count = lax.axis_size("dp")
    seq_len = qkv.shape[1]
    head_size = qkv.shape[3] // 3

    heads = qkv.reshape(seq_len, 3 * head_size)
    query = heads[:, :head_size]
    key_rows = heads[:, head_size : 2 * head_size]
    value_rows = heads[:, 2 * head_size :]
    probs = probs_of(doc_lengths, query, key_rows)

    slab = copy_for_each(out_weight.T, "dp")
    slab = slab.reshape(-1, slab.shape[-1])
    terms = enc_grads[0, 0].reshape(rows, 2, 2, share_cols)
    kept = jnp.where(core == 0, terms[:, :, 0], terms[:, :, 1])
    given = jnp.where(core == 0, terms[:, :, 1], terms[:, :, 0])
    came = lax.ppermute(given, "task", core_swap)
    pair = kept.astype(jnp.float32) + came.astype(jnp.float32)
    mine = jnp.where(far == 0, pair[:, 0], pair[:, 1])
    theirs = jnp.where(far == 0, pair[:, 1], pair[:, 0])
    came = lax.ppermute(theirs.astype(jnp.bfloat16), "task", far_swap)
    summed = mine + came.astype(jnp.float32)

    saved_tok, slab = lax.optimization_barrier((attn_out[0], slab))
    saved_all = copy_for_each(saved_tok, "seq")
    saved_all = saved_all.reshape(seq_len, -1)
    weight = lax.all_gather(slab, "seq", axis=0, tiled=True)

    stream = hidden[0].astype(jnp.float32)
    gain = lax.dynamic_slice_in_dim(final_gain, task_pos * share_cols, share_cols, 0)
    sums = jnp.concatenate(
        [jnp.sum(stream * stream, axis=-1), jnp.sum(gain * summed * stream, axis=-1)]
    )
    sums = sums[None]
    shares = [sums]
    for pairs in (core_swap, far_swap, corner_swap):
        shares.append(lax.ppermute(sums, "task", pairs))
    sums = (shares[0] + shares[1] + shares[2] + shares[3])[0]
    squares, cross_sum = sums[:rows], sums[rows:]
    scale_inv = lax.rsqrt(squares / feature_cols + eps_norm)[:, None]
    cross_mean = cross_sum[:, None] * scale_inv / feature_cols
    resid = (scale_inv * (gain * summed - stream * scale_inv * cross_mean)).astype(jnp.bfloat16)

    beside = lax.ppermute(resid, "task", core_swap)
    across = lax.ppermute(resid, "task", far_swap)
    corner = lax.ppermute(across, "task", core_swap)
    near_first = jnp.where(core == 0, resid, beside)
    near_second = jnp.where(core == 0, beside, resid)
    far_first = jnp.where(core == 0, across, corner)
    far_second = jnp.where(core == 0, corner, across)
    resid_full = jnp.concatenate(
        [
            jnp.where(far == 0, near_first, far_first),
            jnp.where(far == 0, near_second, far_second),
            jnp.where(far == 0, far_first, near_first),
            jnp.where(far == 0, far_second, near_second),
        ],
        axis=1,
    )

    resid_full, saved_all = lax.optimization_barrier((resid_full, saved_all))
    resid_cols = lax.all_to_all(resid_full, "seq", split_axis=1, concat_axis=0, tiled=True)
    grad_block = lax.dot_general(
        resid_cols, saved_all, (((0,), (0,)), ((), ())), preferred_element_type=jnp.float32
    )
    blocks = grad_block.reshape(dp_count, -1, grad_block.shape[-1])
    sent = blocks.astype(jnp.bfloat16)
    dp_pos = lax.axis_index("dp")
    weight_sum = pick(blocks, dp_pos)
    for step in range(1, dp_count):
        ring = [(d, (d + step) % dp_count) for d in range(dp_count)]
        piece = pick(sent, (dp_pos + step) % dp_count)
        piece = lax.ppermute(piece, "dp", ring)
        weight_sum = weight_sum + piece.astype(jnp.float32)
    weight_grad = weight_sum.T

    head_grad = lax.dot_general(
        resid_full, weight, NN, preferred_element_type=jnp.float32
    ).astype(jnp.bfloat16)
    head_grad, resid_cols = lax.optimization_barrier((head_grad, resid_cols))
    upstream = lax.all_to_all(head_grad, "seq", split_axis=1, concat_axis=0, tiled=True)
    saved = lax.dynamic_slice_in_dim(
        saved_all, lax.axis_index("seq") * head_size, head_size, 1
    )
    qkv_grad = grads_of(probs, query, upstream, saved, key_rows, value_rows, key_rows.T)
    return (resid[None], qkv_grad.reshape(1, seq_len, 1, 3 * head_size), weight_grad)


def solution(mesh):
    return jax.shard_map(
        compute,
        mesh=mesh,
        in_specs=(
            P("task", "dp", "seq", None),
            P("dp", "seq", "task"),
            P(),
            P("dp", "seq", "task"),
            P("dp", None, ("task", "seq"), None),
            P("task", ("seq", "dp")),
            P("dp"),
        ),
        out_specs=(
            P("dp", "seq", "task"),
            P("dp", None, ("task", "seq"), None),
            P("task", ("seq", "dp")),
        ),
        check_vma=False,
    )
```

```python
import jax
import jax.numpy as jnp
from jax import lax
from jax.experimental import pallas as pl
from jax.experimental.pallas import tpu as pltpu
from jax.sharding import PartitionSpec as P


eps_norm = 1e-06
core_swap = [(0, 1), (1, 0), (2, 3), (3, 2)]
far_swap = [(0, 2), (2, 0), (1, 3), (3, 1)]
NT = (((1,), (1,)), ((), ()))
NN = (((1,), (0,)), ((), ()))
tile = 256


def probs_kernel(length_ref, q_ref, k_ref, out_ref, held):
    keys = k_ref.shape[0]
    q = q_ref[...]
    length = length_ref[0]
    top = None
    for start in range(0, keys, tile):
        rows = pl.ds(start, tile)
        s = lax.dot_general(k_ref[rows, :], q, NT, preferred_element_type=jnp.float32)
        place = lax.broadcasted_iota(jnp.int32, s.shape, 0) + start
        s = jnp.where(place < length, s, -1e30)
        held[rows, :] = s
        peak = jnp.max(s, axis=0, keepdims=True)
        top = peak if top is None else jnp.maximum(top, peak)
    total = jnp.zeros_like(top)
    for start in range(0, keys, tile):
        rows = pl.ds(start, tile)
        e = jnp.exp(held[rows, :] - top)
        held[rows, :] = e
        total = total + jnp.sum(e, axis=0, keepdims=True)
    share = 1.0 / total
    for start in range(0, keys, tile):
        rows = pl.ds(start, tile)
        out_ref[rows, :] = (held[rows, :] * share).astype(out_ref.dtype)


def probs_of(length, query, key_rows):
    n, size = query.shape
    return pl.pallas_call(
        probs_kernel,
        grid=(n // tile,),
        in_specs=[
            pl.BlockSpec(memory_space=pltpu.SMEM),
            pl.BlockSpec((tile, size), lambda i: (i, 0)),
            pl.BlockSpec((n, size), lambda i: (0, 0)),
        ],
        out_specs=pl.BlockSpec((n, tile), lambda i: (0, i)),
        out_shape=jax.ShapeDtypeStruct((n, n), jnp.bfloat16),
        scratch_shapes=[pltpu.VMEM((n, tile), jnp.float32)],
        cost_estimate=pl.CostEstimate(
            flops=8 * n * n * size, bytes_accessed=2 * n * n, transcendentals=n * n
        ),
        name="probs",
    )(length, query, key_rows)


def grads_kernel(p_ref, q_ref, g_ref, o_ref, k_ref, v_ref, kt_ref, out_ref, dk_acc, dv_acc):
    i = pl.program_id(0)
    keys, size = k_ref.shape
    q = q_ref[...]
    g = g_ref[...]
    prod = g.astype(jnp.float32) * o_ref[...].astype(jnp.float32)
    delta = lax.dot_general(
        jnp.ones((8, size), jnp.float32),
        prod,
        NT,
        precision=lax.Precision.HIGHEST,
        preferred_element_type=jnp.float32,
    )[0:1, :]

    @pl.when(i == 0)
    def _():
        dk_acc[...] = jnp.zeros_like(dk_acc)
        dv_acc[...] = jnp.zeros_like(dv_acc)

    dqt = jnp.zeros((size, tile), jnp.float32)
    for start in range(0, keys, tile):
        rows = pl.ds(start, tile)
        p = p_ref[rows, :]
        dp = lax.dot_general(v_ref[rows, :], g, NT, preferred_element_type=jnp.float32)
        ds = (p.astype(jnp.float32) * (dp - delta)).astype(jnp.bfloat16)
        dv_acc[rows, :] += lax.dot_general(p, g, NN, preferred_element_type=jnp.float32)
        dk_acc[rows, :] += lax.dot_general(ds, q, NN, preferred_element_type=jnp.float32)
        dqt = dqt + lax.dot_general(kt_ref[:, rows], ds, NN, preferred_element_type=jnp.float32)
    out_ref[pl.ds(pl.multiple_of(i * tile, tile), tile), 0:size] = dqt.T.astype(out_ref.dtype)

    @pl.when(i == pl.num_programs(0) - 1)
    def _():
        out_ref[:, size : 2 * size] = dk_acc[...].astype(out_ref.dtype)
        out_ref[:, 2 * size :] = dv_acc[...].astype(out_ref.dtype)


def grads_of(probs, query, upstream, saved, key_rows, value_rows, key_cols):
    n, size = query.shape
    part = pl.BlockSpec((tile, size), lambda i: (i, 0))
    whole = pl.BlockSpec((n, size), lambda i: (0, 0))
    return pl.pallas_call(
        grads_kernel,
        grid=(n // tile,),
        in_specs=[
            pl.BlockSpec((n, tile), lambda i: (0, i)),
            part,
            part,
            part,
            whole,
            whole,
            pl.BlockSpec((size, n), lambda i: (0, 0)),
        ],
        out_specs=pl.BlockSpec((n, 3 * size), lambda i: (0, 0)),
        out_shape=jax.ShapeDtypeStruct((n, 3 * size), jnp.bfloat16),
        scratch_shapes=[pltpu.VMEM((n, size), jnp.float32), pltpu.VMEM((n, size), jnp.float32)],
        cost_estimate=pl.CostEstimate(
            flops=8 * n * n * size, bytes_accessed=2 * n * n, transcendentals=0
        ),
        name="grads",
    )(probs, query, upstream, saved, key_rows, value_rows, key_cols)


def copy_for_each(shard, axis):
    copies = jnp.broadcast_to(shard, (lax.axis_size(axis), *shard.shape))
    return lax.all_to_all(copies, axis, split_axis=0, concat_axis=0, tiled=True)


def compute(enc_grads, hidden, final_gain, attn_out, qkv, out_weight, doc_lengths):
    rows, feature_cols = enc_grads.shape[2:]
    tasks = lax.axis_size("task")
    task_pos = lax.axis_index("task")
    far, core = task_pos // 2, task_pos % 2
    share_cols = feature_cols // tasks
    dp_count = lax.axis_size("dp")
    seq_len = qkv.shape[1]
    head_size = qkv.shape[3] // 3

    dp_pos = lax.axis_index("dp")
    slab = out_weight.T[None, None, None]
    for axis, bit in ((0, 4), (1, 2), (2, 1)):
        other = lax.ppermute(slab, "dp", [(d, d ^ bit) for d in range(dp_count)])
        lower = (dp_pos & bit) == 0
        slab = jnp.concatenate(
            [jnp.where(lower, slab, other), jnp.where(lower, other, slab)], axis=axis
        )
    slab = slab.reshape(-1, slab.shape[-1])
    weight = lax.all_gather(slab, "seq", axis=0, tiled=True)

    heads = qkv.reshape(seq_len, 3 * head_size)
    query = heads[:, :head_size]
    key_rows = heads[:, head_size : 2 * head_size]
    value_rows = heads[:, 2 * head_size :]
    query_after, slab = lax.optimization_barrier((query, slab))
    probs = probs_of(doc_lengths, query_after, key_rows)

    terms = enc_grads[0, 0].reshape(rows, 2, 2, share_cols)
    kept = jnp.where(core == 0, terms[:, :, 0], terms[:, :, 1])
    given = jnp.where(core == 0, terms[:, :, 1], terms[:, :, 0])
    came = lax.ppermute(given, "task", core_swap)
    pair = kept.astype(jnp.float32) + came.astype(jnp.float32)
    mine = jnp.where(far == 0, pair[:, 0], pair[:, 1])
    theirs = jnp.where(far == 0, pair[:, 1], pair[:, 0])
    came = lax.ppermute(theirs.astype(jnp.bfloat16), "task", far_swap)
    summed = mine + came.astype(jnp.float32)

    saved_all = copy_for_each(attn_out[0], "seq")
    saved_all = saved_all.reshape(seq_len, -1)

    stream = hidden[0].astype(jnp.float32)
    gain = lax.dynamic_slice_in_dim(final_gain, task_pos * share_cols, share_cols, 0)
    sums = jnp.concatenate(
        [jnp.sum(stream * stream, axis=-1), jnp.sum(gain * summed * stream, axis=-1)]
    )
    sums = sums[None]
    sums = sums + lax.ppermute(sums, "task", core_swap)
    sums = (sums + lax.ppermute(sums, "task", far_swap))[0]
    squares, cross_sum = sums[:rows], sums[rows:]
    scale_inv = lax.rsqrt(squares / feature_cols + eps_norm)[:, None]
    cross_mean = cross_sum[:, None] * scale_inv / feature_cols
    resid = (scale_inv * (gain * summed - stream * scale_inv * cross_mean)).astype(jnp.bfloat16)

    beside = lax.ppermute(resid, "task", core_swap)
    across = lax.ppermute(resid, "task", far_swap)
    corner = lax.ppermute(across, "task", core_swap)
    near_first = jnp.where(core == 0, resid, beside)
    near_second = jnp.where(core == 0, beside, resid)
    far_first = jnp.where(core == 0, across, corner)
    far_second = jnp.where(core == 0, corner, across)
    resid_full = jnp.concatenate(
        [
            jnp.where(far == 0, near_first, far_first),
            jnp.where(far == 0, near_second, far_second),
            jnp.where(far == 0, far_first, near_first),
            jnp.where(far == 0, far_second, near_second),
        ],
        axis=1,
    )

    resid_full, saved_all = lax.optimization_barrier((resid_full, saved_all))
    resid_cols = lax.all_to_all(resid_full, "seq", split_axis=1, concat_axis=0, tiled=True)
    grad_block = lax.dot_general(
        resid_cols, saved_all, (((0,), (0,)), ((), ())), preferred_element_type=jnp.float32
    )
    total = grad_block.reshape(2, 2, 2, -1, grad_block.shape[-1])
    for axis, bit in ((2, 1), (1, 2), (0, 4)):
        lower = (dp_pos & bit) == 0
        first, second = (
            lax.index_in_dim(total, side, axis, keepdims=True) for side in (0, 1)
        )
        given = jnp.where(lower, second, first).astype(jnp.bfloat16)
        came = lax.ppermute(given, "dp", [(d, d ^ bit) for d in range(dp_count)])
        total = jnp.where(lower, first, second) + came.astype(jnp.float32)
    weight_grad = total.reshape(total.shape[-2:]).T

    head_grad = lax.dot_general(
        resid_full, weight, NN, preferred_element_type=jnp.float32
    ).astype(jnp.bfloat16)
    head_grad, resid_cols = lax.optimization_barrier((head_grad, resid_cols))
    upstream = lax.all_to_all(head_grad, "seq", split_axis=1, concat_axis=0, tiled=True)
    saved = lax.dynamic_slice_in_dim(
        saved_all, lax.axis_index("seq") * head_size, head_size, 1
    )
    qkv_grad = grads_of(probs, query, upstream, saved, key_rows, value_rows, key_rows.T)
    return (resid[None], qkv_grad.reshape(1, seq_len, 1, 3 * head_size), weight_grad)


def solution(mesh):
    return jax.shard_map(
        compute,
        mesh=mesh,
        in_specs=(
            P("task", "dp", "seq", None),
            P("dp", "seq", "task"),
            P(),
            P("dp", "seq", "task"),
            P("dp", None, ("task", "seq"), None),
            P("task", ("seq", "dp")),
            P("dp"),
        ),
        out_specs=(
            P("dp", "seq", "task"),
            P("dp", None, ("task", "seq"), None),
            P("task", ("seq", "dp")),
        ),
        check_vma=False,
    )
```

```python
import jax
import jax.numpy as jnp
from jax import lax
from jax.experimental import pallas as pl
from jax.experimental.layout import Layout, with_layout_constraint
from jax.experimental.pallas import tpu as pltpu
from jax.sharding import PartitionSpec as P


eps_norm = 1e-06
core_swap = [(0, 1), (1, 0), (2, 3), (3, 2)]
far_swap = [(0, 2), (2, 0), (1, 3), (3, 1)]
NT = (((1,), (1,)), ((), ()))
NN = (((1,), (0,)), ((), ()))
tile = 256
wide = 512


def probs_kernel(length_ref, q_ref, k_ref, out_ref, held):
    keys = k_ref.shape[0]
    q = q_ref[...]
    length = length_ref[0]
    top = None
    for start in range(0, keys, tile):
        rows = pl.ds(start, tile)
        s = lax.dot_general(k_ref[rows, :], q, NT, preferred_element_type=jnp.float32)
        place = lax.broadcasted_iota(jnp.int32, s.shape, 0) + start
        s = jnp.where(place < length, s, -1e30)
        held[rows, :] = s
        peak = jnp.max(s, axis=0, keepdims=True)
        top = peak if top is None else jnp.maximum(top, peak)
    total = jnp.zeros_like(top)
    for start in range(0, keys, tile):
        rows = pl.ds(start, tile)
        e = jnp.exp(held[rows, :] - top)
        held[rows, :] = e
        total = total + jnp.sum(e, axis=0, keepdims=True)
    share = 1.0 / total
    for start in range(0, keys, tile):
        rows = pl.ds(start, tile)
        out_ref[rows, :] = (held[rows, :] * share).astype(out_ref.dtype)


def probs_of(length, query, key_rows):
    n, size = query.shape
    return pl.pallas_call(
        probs_kernel,
        grid=(n // tile,),
        in_specs=[
            pl.BlockSpec(memory_space=pltpu.SMEM),
            pl.BlockSpec((tile, size), lambda i: (i, 0)),
            pl.BlockSpec((n, size), lambda i: (0, 0)),
        ],
        out_specs=pl.BlockSpec((n, tile), lambda i: (0, i)),
        out_shape=jax.ShapeDtypeStruct((n, n), jnp.bfloat16),
        scratch_shapes=[pltpu.VMEM((n, tile), jnp.float32)],
        cost_estimate=pl.CostEstimate(
            flops=8 * n * n * size, bytes_accessed=2 * n * n, transcendentals=n * n
        ),
        name="probs",
    )(length, query, key_rows)


def grads_kernel(p_ref, q_ref, g_ref, o_ref, v_ref, k_ref, out_ref, dk_acc, dv_acc):
    i = pl.program_id(0)
    keys, size = v_ref.shape
    q = q_ref[...]
    g = jnp.concatenate([g_ref[j] for j in range(g_ref.shape[0])], axis=1)
    prod = g.astype(jnp.float32) * o_ref[...].astype(jnp.float32)
    delta = jnp.sum(prod, axis=0, keepdims=True)

    @pl.when(i == 0)
    def _():
        dk_acc[...] = jnp.zeros_like(dk_acc)
        dv_acc[...] = jnp.zeros_like(dv_acc)

    dq = jnp.zeros((size, wide), jnp.float32)
    for start in range(0, keys, tile):
        rows = pl.ds(start, tile)
        p = p_ref[rows, :]
        dp = lax.dot_general(v_ref[rows, :], g, NN, preferred_element_type=jnp.float32)
        ds = (p.astype(jnp.float32) * (dp - delta)).astype(jnp.bfloat16)
        dv_acc[:, rows] += lax.dot_general(g, p, NT, preferred_element_type=jnp.float32)
        dk_acc[:, rows] += lax.dot_general(q, ds, NT, preferred_element_type=jnp.float32)
        dq = dq + lax.dot_general(k_ref[:, rows], ds, NN, preferred_element_type=jnp.float32)
    out_ref[0:size, pl.ds(pl.multiple_of(i * wide, wide), wide)] = dq.astype(out_ref.dtype)

    @pl.when(i == pl.num_programs(0) - 1)
    def _():
        out_ref[size : 2 * size, :] = dk_acc[...].astype(out_ref.dtype)
        out_ref[2 * size :, :] = dv_acc[...].astype(out_ref.dtype)


def grads_of(probs, query_cols, upstream, saved_cols, value_rows, key_cols):
    n, size = value_rows.shape
    each = wide // upstream.shape[2]
    part = pl.BlockSpec((size, wide), lambda i: (0, i))
    return pl.pallas_call(
        grads_kernel,
        grid=(n // wide,),
        in_specs=[
            pl.BlockSpec((n, wide), lambda i: (0, i)),
            part,
            pl.BlockSpec((each, size, upstream.shape[2]), lambda i: (i, 0, 0)),
            part,
            pl.BlockSpec((n, size), lambda i: (0, 0)),
            pl.BlockSpec((size, n), lambda i: (0, 0)),
        ],
        out_specs=pl.BlockSpec((3 * size, n), lambda i: (0, 0)),
        out_shape=jax.ShapeDtypeStruct((3 * size, n), jnp.bfloat16),
        scratch_shapes=[pltpu.VMEM((size, n), jnp.float32), pltpu.VMEM((size, n), jnp.float32)],
        cost_estimate=pl.CostEstimate(
            flops=8 * n * n * size, bytes_accessed=2 * n * n, transcendentals=0
        ),
        name="grads",
    )(probs, query_cols, upstream, saved_cols, value_rows, key_cols)


def copy_for_each(shard, axis):
    copies = jnp.broadcast_to(shard, (lax.axis_size(axis), *shard.shape))
    return lax.all_to_all(copies, axis, split_axis=0, concat_axis=0, tiled=True)


def by_rows(array):
    return with_layout_constraint(array, Layout(major_to_minor=tuple(range(array.ndim))))


def compute(enc_grads, hidden, final_gain, attn_out, qkv, out_weight, doc_lengths):
    rows, feature_cols = enc_grads.shape[2:]
    tasks = lax.axis_size("task")
    task_pos = lax.axis_index("task")
    far, core = task_pos // 2, task_pos % 2
    share_cols = feature_cols // tasks
    seq_count = lax.axis_size("seq")
    dp_count = lax.axis_size("dp")
    seq_len = qkv.shape[1]
    head_size = qkv.shape[3] // 3

    dp_pos = lax.axis_index("dp")
    slab = out_weight.T[None, None, None]
    for axis, bit in ((0, 4), (1, 2), (2, 1)):
        other = lax.ppermute(slab, "dp", [(d, d ^ bit) for d in range(dp_count)])
        lower = (dp_pos & bit) == 0
        slab = jnp.concatenate(
            [jnp.where(lower, slab, other), jnp.where(lower, other, slab)], axis=axis
        )
    slab = slab.reshape(-1, slab.shape[-1])
    weight = lax.all_gather(slab, "seq", axis=0, tiled=True)

    heads = qkv.reshape(seq_len, 3 * head_size)
    query = heads[:, :head_size]
    key_rows = heads[:, head_size : 2 * head_size]
    value_rows = heads[:, 2 * head_size :]
    query_cols, key_cols = heads.T[:head_size], heads.T[head_size : 2 * head_size]
    query, key_rows, value_rows, query_cols, key_cols, slab = lax.optimization_barrier(
        (query, key_rows, value_rows, query_cols, key_cols, slab)
    )
    probs = probs_of(doc_lengths, query, key_rows)

    terms = enc_grads[0, 0].reshape(rows, 2, 2, share_cols)
    kept = jnp.where(core == 0, terms[:, :, 0], terms[:, :, 1])
    given = jnp.where(core == 0, terms[:, :, 1], terms[:, :, 0])
    came = lax.ppermute(given, "task", core_swap)
    pair = kept.astype(jnp.float32) + came.astype(jnp.float32)
    mine = jnp.where(far == 0, pair[:, 0], pair[:, 1])
    theirs = jnp.where(far == 0, pair[:, 1], pair[:, 0])
    came = lax.ppermute(theirs.astype(jnp.bfloat16), "task", far_swap)
    summed = mine + came.astype(jnp.float32)

    saved_all = by_rows(copy_for_each(by_rows(attn_out[0]), "seq"))
    saved_all = by_rows(saved_all.reshape(seq_len, -1))

    stream = hidden[0].astype(jnp.float32)
    gain = lax.dynamic_slice_in_dim(final_gain, task_pos * share_cols, share_cols, 0)
    sums = jnp.concatenate(
        [jnp.sum(stream * stream, axis=-1), jnp.sum(gain * summed * stream, axis=-1)]
    )
    sums = sums[None]
    sums = sums + lax.ppermute(sums, "task", core_swap)
    sums = (sums + lax.ppermute(sums, "task", far_swap))[0]
    squares, cross_sum = sums[:rows], sums[rows:]
    scale_inv = lax.rsqrt(squares / feature_cols + eps_norm)[:, None]
    cross_mean = cross_sum[:, None] * scale_inv / feature_cols
    resid = (scale_inv * (gain * summed - stream * scale_inv * cross_mean)).astype(jnp.bfloat16)

    beside = lax.ppermute(resid, "task", core_swap)
    across = lax.ppermute(resid, "task", far_swap)
    corner = lax.ppermute(across, "task", core_swap)
    near_first = jnp.where(core == 0, resid, beside)
    near_second = jnp.where(core == 0, beside, resid)
    far_first = jnp.where(core == 0, across, corner)
    far_second = jnp.where(core == 0, corner, across)
    resid_full = jnp.concatenate(
        [
            jnp.where(far == 0, near_first, far_first),
            jnp.where(far == 0, near_second, far_second),
            jnp.where(far == 0, far_first, near_first),
            jnp.where(far == 0, far_second, near_second),
        ],
        axis=1,
    )

    saved_cols = lax.dynamic_slice_in_dim(
        saved_all, lax.axis_index("seq") * head_size, head_size, 1
    )
    saved_cols = lax.optimization_barrier(saved_cols).T
    resid_full, saved_all, saved_cols = lax.optimization_barrier(
        (resid_full, saved_all, saved_cols)
    )
    resid_cols = lax.all_to_all(resid_full, "seq", split_axis=1, concat_axis=0, tiled=True)
    grad_block = lax.dot_general(
        resid_cols, saved_all, (((0,), (0,)), ((), ())), preferred_element_type=jnp.float32
    )
    total = grad_block.reshape(2, 2, 2, -1, grad_block.shape[-1])
    for axis, bit in ((2, 1), (1, 2), (0, 4)):
        lower = (dp_pos & bit) == 0
        first, second = (
            lax.index_in_dim(total, side, axis, keepdims=True) for side in (0, 1)
        )
        given = jnp.where(lower, second, first).astype(jnp.bfloat16)
        came = lax.ppermute(given, "dp", [(d, d ^ bit) for d in range(dp_count)])
        total = jnp.where(lower, first, second) + came.astype(jnp.float32)
    weight_grad = total.reshape(total.shape[-2:]).T

    head_grad = lax.dot_general(
        resid_full, weight, NN, preferred_element_type=jnp.float32
    ).astype(jnp.bfloat16)
    head_grad, resid_cols = lax.optimization_barrier((head_grad, resid_cols))
    head_grad = head_grad.T.reshape(seq_count, head_size, rows)
    upstream = lax.all_to_all(head_grad, "seq", split_axis=0, concat_axis=0, tiled=True)
    qkv_grad = grads_of(probs, query_cols, upstream, saved_cols, value_rows, key_cols)
    return (resid[None], qkv_grad.T.reshape(1, seq_len, 1, 3 * head_size), weight_grad)


def solution(mesh):
    return jax.shard_map(
        compute,
        mesh=mesh,
        in_specs=(
            P("task", "dp", "seq", None),
            P("dp", "seq", "task"),
            P(),
            P("dp", "seq", "task"),
            P("dp", None, ("task", "seq"), None),
            P("task", ("seq", "dp")),
            P("dp"),
        ),
        out_specs=(
            P("dp", "seq", "task"),
            P("dp", None, ("task", "seq"), None),
            P("task", ("seq", "dp")),
        ),
        check_vma=False,
    )
```

```python
import jax
import jax.numpy as jnp
from jax import lax
from jax.experimental import pallas as pl
from jax.experimental.layout import Layout, with_layout_constraint
from jax.experimental.pallas import tpu as pltpu
from jax.sharding import PartitionSpec as P


eps_norm = 1e-06
core_swap = [(0, 1), (1, 0), (2, 3), (3, 2)]
far_swap = [(0, 2), (2, 0), (1, 3), (3, 1)]
NT = (((1,), (1,)), ((), ()))
NN = (((1,), (0,)), ((), ()))
tile = 256
wide = 512


def probs_kernel(length_ref, q_ref, k_ref, out_ref, held):
    keys = k_ref.shape[0]
    q = q_ref[...]
    length = length_ref[0]
    top = None
    for start in range(0, keys, tile):
        rows = pl.ds(start, tile)
        s = lax.dot_general(k_ref[rows, :], q, NT, preferred_element_type=jnp.float32)
        place = lax.broadcasted_iota(jnp.int32, s.shape, 0) + start
        s = jnp.where(place < length, s, -1e30)
        held[rows, :] = s
        peak = jnp.max(s, axis=0, keepdims=True)
        top = peak if top is None else jnp.maximum(top, peak)
    total = jnp.zeros_like(top)
    for start in range(0, keys, tile):
        rows = pl.ds(start, tile)
        e = jnp.exp(held[rows, :] - top)
        held[rows, :] = e
        total = total + jnp.sum(e, axis=0, keepdims=True)
    share = 1.0 / total
    for start in range(0, keys, tile):
        rows = pl.ds(start, tile)
        out_ref[rows, :] = (held[rows, :] * share).astype(out_ref.dtype)


def probs_of(length, query, key_rows):
    n, size = query.shape
    return pl.pallas_call(
        probs_kernel,
        grid=(n // tile,),
        in_specs=[
            pl.BlockSpec(memory_space=pltpu.SMEM),
            pl.BlockSpec((tile, size), lambda i: (i, 0)),
            pl.BlockSpec((n, size), lambda i: (0, 0)),
        ],
        out_specs=pl.BlockSpec((n, tile), lambda i: (0, i)),
        out_shape=jax.ShapeDtypeStruct((n, n), jnp.bfloat16),
        scratch_shapes=[pltpu.VMEM((n, tile), jnp.float32)],
        cost_estimate=pl.CostEstimate(
            flops=8 * n * n * size, bytes_accessed=2 * n * n, transcendentals=n * n
        ),
        name="probs",
    )(length, query, key_rows)


def grads_kernel(p_ref, q_ref, g_ref, o_ref, v_ref, k_ref, out_ref, dk_acc, dv_acc):
    i = pl.program_id(0)
    keys, size = v_ref.shape
    q = q_ref[...]
    g = jnp.concatenate([g_ref[j] for j in range(g_ref.shape[0])], axis=1)
    prod = g.astype(jnp.float32) * o_ref[...].astype(jnp.float32)
    delta = jnp.sum(prod, axis=0, keepdims=True)

    @pl.when(i == 0)
    def _():
        dk_acc[...] = jnp.zeros_like(dk_acc)
        dv_acc[...] = jnp.zeros_like(dv_acc)

    dq = jnp.zeros((size, wide), jnp.float32)
    for start in range(0, keys, tile):
        rows = pl.ds(start, tile)
        p = p_ref[rows, :]
        dp = lax.dot_general(v_ref[rows, :], g, NN, preferred_element_type=jnp.float32)
        ds = (p.astype(jnp.float32) * (dp - delta)).astype(jnp.bfloat16)
        dv_acc[:, rows] += lax.dot_general(g, p, NT, preferred_element_type=jnp.float32)
        dk_acc[:, rows] += lax.dot_general(q, ds, NT, preferred_element_type=jnp.float32)
        dq = dq + lax.dot_general(k_ref[:, rows], ds, NN, preferred_element_type=jnp.float32)
    out_ref[0:size, pl.ds(pl.multiple_of(i * wide, wide), wide)] = dq.astype(out_ref.dtype)

    @pl.when(i == pl.num_programs(0) - 1)
    def _():
        out_ref[size : 2 * size, :] = dk_acc[...].astype(out_ref.dtype)
        out_ref[2 * size :, :] = dv_acc[...].astype(out_ref.dtype)


def grads_of(probs, query_cols, upstream, saved_cols, value_rows, key_cols):
    n, size = value_rows.shape
    each = wide // upstream.shape[2]
    part = pl.BlockSpec((size, wide), lambda i: (0, i))
    return pl.pallas_call(
        grads_kernel,
        grid=(n // wide,),
        in_specs=[
            pl.BlockSpec((n, wide), lambda i: (0, i)),
            part,
            pl.BlockSpec((each, size, upstream.shape[2]), lambda i: (i, 0, 0)),
            part,
            pl.BlockSpec((n, size), lambda i: (0, 0)),
            pl.BlockSpec((size, n), lambda i: (0, 0)),
        ],
        out_specs=pl.BlockSpec((3 * size, n), lambda i: (0, 0)),
        out_shape=jax.ShapeDtypeStruct((3 * size, n), jnp.bfloat16),
        scratch_shapes=[pltpu.VMEM((size, n), jnp.float32), pltpu.VMEM((size, n), jnp.float32)],
        cost_estimate=pl.CostEstimate(
            flops=8 * n * n * size, bytes_accessed=2 * n * n, transcendentals=0
        ),
        name="grads",
    )(probs, query_cols, upstream, saved_cols, value_rows, key_cols)


def by_rows(array):
    return with_layout_constraint(array, Layout(major_to_minor=tuple(range(array.ndim))))


def compute(enc_grads, hidden, final_gain, attn_out, qkv, out_weight, doc_lengths):
    rows, feature_cols = enc_grads.shape[2:]
    tasks = lax.axis_size("task")
    task_pos = lax.axis_index("task")
    far, core = task_pos // 2, task_pos % 2
    share_cols = feature_cols // tasks
    seq_count = lax.axis_size("seq")
    dp_count = lax.axis_size("dp")
    seq_len = qkv.shape[1]
    head_size = qkv.shape[3] // 3

    dp_pos = lax.axis_index("dp")
    slab = out_weight.T[None, None, None]
    for axis, bit in ((0, 4), (1, 2), (2, 1)):
        other = lax.ppermute(slab, "dp", [(d, d ^ bit) for d in range(dp_count)])
        lower = (dp_pos & bit) == 0
        slab = jnp.concatenate(
            [jnp.where(lower, slab, other), jnp.where(lower, other, slab)], axis=axis
        )
    slab = slab.reshape(-1, slab.shape[-1])
    weight = lax.all_gather(slab, "seq", axis=0, tiled=True)

    heads = qkv.reshape(seq_len, 3 * head_size)
    query = heads[:, :head_size]
    key_rows = heads[:, head_size : 2 * head_size]
    value_rows = heads[:, 2 * head_size :]
    query_cols, key_cols = heads.T[:head_size], heads.T[head_size : 2 * head_size]
    query, key_rows, value_rows, query_cols, key_cols = lax.optimization_barrier(
        (query, key_rows, by_rows(value_rows), query_cols, key_cols)
    )
    probs = probs_of(doc_lengths, query, key_rows)

    terms = enc_grads[0, 0].reshape(rows, 2, 2, share_cols)
    kept = jnp.where(core == 0, terms[:, :, 0], terms[:, :, 1])
    given = jnp.where(core == 0, terms[:, :, 1], terms[:, :, 0])
    came = lax.ppermute(given, "task", core_swap)
    pair = kept.astype(jnp.float32) + came.astype(jnp.float32)
    mine = jnp.where(far == 0, pair[:, 0], pair[:, 1])
    theirs = jnp.where(far == 0, pair[:, 1], pair[:, 0])
    came = lax.ppermute(theirs.astype(jnp.bfloat16), "task", far_swap)
    summed = mine + came.astype(jnp.float32)

    saved_all = by_rows(lax.all_gather(attn_out[0], "seq", axis=0, tiled=True))

    stream = hidden[0].astype(jnp.float32)
    gain = lax.dynamic_slice_in_dim(final_gain, task_pos * share_cols, share_cols, 0)
    sums = jnp.concatenate(
        [jnp.sum(stream * stream, axis=-1), jnp.sum(gain * summed * stream, axis=-1)]
    )
    sums = sums[None]
    sums = sums + lax.ppermute(sums, "task", core_swap)
    sums = (sums + lax.ppermute(sums, "task", far_swap))[0]
    squares, cross_sum = sums[:rows], sums[rows:]
    scale_inv = lax.rsqrt(squares / feature_cols + eps_norm)[:, None]
    cross_mean = cross_sum[:, None] * scale_inv / feature_cols
    resid = (scale_inv * (gain * summed - stream * scale_inv * cross_mean)).astype(jnp.bfloat16)

    beside = lax.ppermute(resid, "task", core_swap)
    across = lax.ppermute(resid, "task", far_swap)
    corner = lax.ppermute(across, "task", core_swap)
    near_first = jnp.where(core == 0, resid, beside)
    near_second = jnp.where(core == 0, beside, resid)
    far_first = jnp.where(core == 0, across, corner)
    far_second = jnp.where(core == 0, corner, across)
    resid_full = jnp.concatenate(
        [
            jnp.where(far == 0, near_first, far_first),
            jnp.where(far == 0, near_second, far_second),
            jnp.where(far == 0, far_first, near_first),
            jnp.where(far == 0, far_second, near_second),
        ],
        axis=1,
    )

    saved_cols = lax.dynamic_slice_in_dim(
        saved_all, lax.axis_index("seq") * head_size, head_size, 1
    )
    saved_cols = lax.optimization_barrier(saved_cols).T
    resid_full, saved_all, saved_cols = lax.optimization_barrier(
        (resid_full, saved_all, saved_cols)
    )
    resid_cols = lax.all_to_all(resid_full, "seq", split_axis=1, concat_axis=0, tiled=True)
    grad_block = lax.dot_general(
        resid_cols, saved_all, (((0,), (0,)), ((), ())), preferred_element_type=jnp.float32
    )
    total = grad_block.reshape(2, 2, 2, -1, grad_block.shape[-1])
    for axis, bit in ((2, 1), (1, 2), (0, 4)):
        lower = (dp_pos & bit) == 0
        first, second = (
            lax.index_in_dim(total, side, axis, keepdims=True) for side in (0, 1)
        )
        given = jnp.where(lower, second, first).astype(jnp.bfloat16)
        came = lax.ppermute(given, "dp", [(d, d ^ bit) for d in range(dp_count)])
        total = jnp.where(lower, first, second) + came.astype(jnp.float32)
    weight_grad = total.reshape(total.shape[-2:]).T

    head_grad = lax.dot_general(
        resid_full, weight, NN, preferred_element_type=jnp.float32
    ).astype(jnp.bfloat16)
    head_grad, resid_cols = lax.optimization_barrier((head_grad, resid_cols))
    head_grad = head_grad.T.reshape(seq_count, head_size, rows)
    upstream = lax.all_to_all(head_grad, "seq", split_axis=0, concat_axis=0, tiled=True)
    qkv_grad = grads_of(probs, query_cols, upstream, saved_cols, value_rows, key_cols)
    return (resid[None], qkv_grad.T.reshape(1, seq_len, 1, 3 * head_size), weight_grad)


def solution(mesh):
    return jax.shard_map(
        compute,
        mesh=mesh,
        in_specs=(
            P("task", "dp", "seq", None),
            P("dp", "seq", "task"),
            P(),
            P("dp", "seq", "task"),
            P("dp", None, ("task", "seq"), None),
            P("task", ("seq", "dp")),
            P("dp"),
        ),
        out_specs=(
            P("dp", "seq", "task"),
            P("dp", None, ("task", "seq"), None),
            P("task", ("seq", "dp")),
        ),
        check_vma=False,
    )
```
